32 devices in a mesh: blk: 8 (over z, x), dp: 4 (over y, core).
Axes of the slice: x: 2, y: 2, z: 4, core: 2. Of those that a mesh axis runs over, the one named last changes fastest.
Arguments:
- images: bfloat16 [4096, 768], P(('dp', 'blk')), parts along dimension 0, may hold values from -4 to 4
- texts: bfloat16 [4096, 768], P(('dp', 'blk')), parts along dimension 0, may hold values from -4 to 4
- scale: float32 [1], replicated, may hold values from 10 to 20
- cotangent: float32 [2, 4096], P(None, ('dp', 'blk')), parts along dimension 1, may hold values from 0.5 to 2
Outputs:
- row_losses: float32 [2, 4096], P(None, ('dp', 'blk')), parts along dimension 1
- grad_images: float32 [4096, 768], P(('dp', 'blk')), parts along dimension 0
- grad_texts: float32 [4096, 768], P(('dp', 'blk')), parts along dimension 0
The draws below stay inside these ranges and needn't reach their ends.
There are 4 independent parts, one for each index of `dp`. The reference program is written for one: setup_inputs(seed, part) draws one part's arguments, and reference() takes and returns one part's arrays. A program takes and returns all parts, laid end to end along the dimension named above; an argument that names none is the same for every part. Nothing has to cross between parts.
All inputs are finite; a program needn't handle non-finite values.
Results may differ from the reference program's by a relative error of at most 0.0019.
Values may be sent and summed in bfloat16 or wider, within the bound.
A program may use at most 64 MiB of HBM per device.

```python
import math
import jax
import jax.numpy as jnp
from jax import lax

WIDTH = 768
BATCH = 1024


def embed_pair(key):
    base_key = jax.random.fold_in(key, 11)
    keys = jax.random.split(base_key, 2)
    images = jnp.clip(0.05 * jax.random.normal(keys[0], (BATCH, WIDTH), jnp.float32), -0.3, 0.3)
    texts = jnp.clip(0.05 * jax.random.normal(keys[1], (BATCH, WIDTH), jnp.float32), -0.3, 0.3)
    return (jnp.clip(images, -4.0, 4.0), jnp.clip(texts, -4.0, 4.0))


def draw_images(key, part):
    return embed_pair(key)[0].astype(jnp.bfloat16)


def draw_texts(key, part):
    return embed_pair(key)[1].astype(jnp.bfloat16)


def shard_levels(rng, dims, pieces, least, largest):
    factor_of = 1.0
    for axis_at, parts in pieces:
        draws = jax.random.uniform(jax.random.fold_in(jax.random.fold_in(rng, 6), axis_at), (parts,), jnp.float32, least / len(pieces), largest / len(pieces))
        factor_of = factor_of * jnp.repeat(jnp.exp(draws), dims[axis_at] // parts).reshape((-1,) + (1,) * (len(dims) - 1 - axis_at))
    return factor_of


def setup_inputs(seed: int = 0, part: int = 0) -> dict:
    key_of = jax.random.split(jax.random.key(seed), 5)
    own_keys = jax.random.split(jax.random.fold_in(key_of[4], part), 5)
    images = draw_images(jax.random.fold_in(jax.random.fold_in(key_of[4], part), 71), part)
    texts = draw_texts(jax.random.fold_in(jax.random.fold_in(key_of[4], part), 71), part)
    scale = jnp.clip(jax.random.uniform(key_of[2], (1,), jnp.float32, 10.0, 20.0), 10.0, 20.0)
    cotangent = jnp.clip(jnp.exp(math.log(2.0) - 1.3862944 * jax.random.uniform(own_keys[3], (2, BATCH), jnp.float32) ** shard_levels(own_keys[3], (2, BATCH), ((1, 8),), -0.2, 0.2)), 0.5, 2.0)
    return {"images": images, "texts": texts, "scale": scale, "cotangent": cotangent}


def lse_blocks(left, right, logit_scale, span):
    def one_block(block):
        scores = logit_scale * jnp.dot(block, right.T, preferred_element_type=jnp.float32)
        top_value = jnp.max(scores, axis=1, keepdims=True)
        return (top_value + jnp.log(jnp.sum(jnp.exp(scores - top_value), axis=1, keepdims=True)))[:, 0]
    blocked = left.reshape(left.shape[0] // span, span, left.shape[1])
    return lax.map(one_block, blocked).reshape(left.shape[0])


def grad_blocks(left, right, own_lse, own_cot, other_lse, other_cot, logit_scale, span):
    def one_block(packed):
        block, lse_block, cot_block = packed
        scores = logit_scale * jnp.dot(block, right.T, preferred_element_type=jnp.float32)
        weights = cot_block[:, None] * jnp.exp(scores - lse_block[:, None]) + other_cot[None, :] * jnp.exp(scores - other_lse[None, :])
        return jnp.dot(weights.astype(jnp.bfloat16), right, preferred_element_type=jnp.float32)
    count = left.shape[0] // span
    packed = (left.reshape(count, span, left.shape[1]), own_lse.reshape(count, span), own_cot.reshape(count, span))
    return lax.map(one_block, packed).reshape(left.shape[0], right.shape[1])


def reference(images, texts, scale, cotangent):
    logit_scale = scale[0]
    span = math.gcd(images.shape[0], 512)
    row_lse = lse_blocks(images, texts, logit_scale, span)
    col_lse = lse_blocks(texts, images, logit_scale, span)
    matched = logit_scale * jnp.sum(images.astype(jnp.float32) * texts.astype(jnp.float32), axis=1)
    row_losses = jnp.stack([row_lse - matched, col_lse - matched])
    cot_rows = cotangent[0]
    cot_cols = cotangent[1]
    both_cot = (cot_rows + cot_cols)[:, None]
    image_terms = grad_blocks(images, texts, row_lse, cot_rows, col_lse, cot_cols, logit_scale, span)
    text_terms = grad_blocks(texts, images, col_lse, cot_cols, row_lse, cot_rows, logit_scale, span)
    grad_images = logit_scale * (image_terms - both_cot * texts.astype(jnp.float32))
    grad_texts = logit_scale * (text_terms - both_cot * images.astype(jnp.float32))
    return row_losses, grad_images, grad_texts
```

```python
import jax
import jax.numpy as jnp
from jax import lax
from jax.experimental import pallas as pl
from jax.experimental.pallas import tpu as pltpu
from jax.sharding import PartitionSpec as P

LANES = 128
MESH = pl.DeviceIdType.MESH

SLOTS = (
    ((0, 0), (0, 1), (1, 0), (1, 1), (2, 0), (2, 1), (3, 0), (3, 1)),
    ((1, 0), (1, 1), (0, 0), (2, 0), (0, 1), (3, 0), (2, 1), (3, 1)),
)
LINE = len(SLOTS[0]) // 2
PHASES = (
    (
        [
            ("I", (0, 1), "i"), ("I", (1, 0), "x"), ("T", (0, 1), "i"), ("T", (1, 0), "x"),
        ],
        [("I", (1, 1), ""), ("I", (2, 0), "x"), ("T", (1, 1), ""), ("T", (2, 0), "x")],
        [("I", (2, 1), ""), ("I", (3, 0), "x"), ("T", (2, 1), ""), ("T", (3, 0), "")],
        [("I", (3, 1), ""), ("T", (3, 1), "")],
    ),
    (
        [
            ("I", (1, 1), ""), ("I", (0, 0), "i"), ("I", (2, 0), "ox"),
            ("T", (1, 1), ""), ("T", (0, 0), "i"), ("T", (2, 0), "ox"),
        ],
        [
            ("I", (0, 1), ""), ("I", (3, 0), "o"), ("T", (0, 1), ""),
            ("T", (3, 0), "ox"), ("I", (3, 0), "X"),
        ],
        [("I", (2, 1), ""), ("T", (2, 1), "")],
        [("T", (3, 1), "o"), ("I", (3, 1), "")],
    ),
)
GROUPS = ((0, 1), (1, 3), (3, 5), (5, 7), (7, 8))
OWN_WAYS = ("ix", "iox")


def landing(half, block, way):
    place, other = block
    if way == "x":
        return half, (place, 1 - other)
    if way == "o":
        return half - 1, block
    if half == LINE // 2 - 1:
        return half, (LINE - 1 - place, other)
    return half + 1, block


def as_column(row, rows):
    return jnp.transpose(jnp.broadcast_to(row, (LANES, rows)))


def fold(top_ref, sum_ref, tile, low, high, fresh):
    top = jnp.max(tile, axis=0, keepdims=True)
    if fresh:
        sum_ref[:, low:high] = jnp.sum(jnp.exp(tile - top), axis=0, keepdims=True)
    else:
        before = top_ref[:, low:high]
        top = jnp.maximum(before, top)
        sum_ref[:, low:high] = sum_ref[:, low:high] * jnp.exp(before - top) + jnp.sum(
            jnp.exp(tile - top), axis=0, keepdims=True
        )
    top_ref[:, low:high] = top


def kernel(
    scale_ref, images_ref, texts_ref, cot_ref, losses_ref, grad_images_ref, grad_texts_ref,
    all_images, all_texts, all_cot, strip_i, strip_t, top_r, sum_r, top_c, sum_c, weights_i, weights_t,
    send_sem, recv_sem,
):
    rows, width = images_ref.shape
    me = lax.axis_index("blk")
    place, column = me // 2, lax.rem(me, 2)
    upper = place // (LINE // 2)
    step = 1 - 2 * upper
    from_end = place + upper * (LINE - 1 - 2 * place)
    peers = {
        "x": place * 2 + 1 - column,
        "i": (place + step) * 2 + column,
        "o": (place - step) * 2 + column,
    }
    kinds = "ITC"

    def part(kind, slot):
        if kind == "C":
            return all_cot.at[slot]
        return (all_images if kind == "I" else all_texts).at[pl.ds(slot * rows, rows)]

    def copy(half, kind, block, way):
        slot = SLOTS[half].index(block)
        there, name = landing(half, block, way)
        own = {"I": images_ref, "T": texts_ref, "C": cot_ref}[kind]
        target = SLOTS[there].index(name)
        at = kinds.index(kind)
        return pltpu.make_async_remote_copy(
            src_ref=own if slot == 0 else part(kind, slot),
            dst_ref=part(kind, target),
            send_sem=send_sem.at[at, slot, "xio".index(way)],
            recv_sem=recv_sem.at[at, target],
            device_id={"blk": peers[way]},
            device_id_type=MESH,
        )

    def arrived(half, kind, block):
        slot = SLOTS[half].index(block)
        at = kinds.index(kind)
        pltpu.make_async_remote_copy(
            src_ref=part(kind, slot),
            dst_ref=part(kind, slot),
            send_sem=send_sem.at[at, slot, 0],
            recv_sem=recv_sem.at[at, slot],
            device_id={"blk": peers["x"]},
            device_id_type=MESH,
        ).wait_recv()

    def both(kind):
        return ("C", "T") if kind == "T" else ("I",)

    sent = ([], [])

    def phase(number):
        for half in range(LINE // 2):

            @pl.when(from_end == half)
            def _():
                for kind, block, ways in PHASES[half][number]:
                    for each in both(kind):
                        if ways != "X":
                            arrived(half, each, block)
                        for way in ways.lower():
                            one = (half, each, block, way)
                            copy(*one).start()
                            sent[half].append(one)

    barrier = pltpu.get_barrier_semaphore()
    for half in range(LINE // 2):

        @pl.when(from_end == half)
        def _():
            for way in OWN_WAYS[half]:
                pl.semaphore_signal(barrier, inc=1, device_id={"blk": peers[way]}, device_id_type=MESH)
            pl.semaphore_wait(barrier, len(OWN_WAYS[half]))
            for kind in "ICT":
                for way in OWN_WAYS[half]:
                    one = (half, kind, SLOTS[half][0], way)
                    copy(*one).start()
                    sent[half].append(one)

    scale = scale_ref[0]
    all_images[0:rows, :] = images_ref[...]
    all_texts[0:rows, :] = texts_ref[...]

    def scores(left, right):
        return scale * dot_rows(left, right)

    def accumulate(left, right, strip, top, total, low, high):
        old, new = low * rows, high * rows
        tile = scores(left[old:new, :], right[0:new, :])
        fold(top, total, tile[:, old:], old, new, True)
        if low == 0:
            strip[:, old:new] = tile
            return
        fold(top, total, tile[:, :old], 0, old, False)
        tile = scores(left[0:old, :], right[old:new, :])
        strip[:, old:new] = tile[0:rows, :]
        fold(top, total, tile, old, new, False)

    for number, (low, high) in enumerate(GROUPS):
        if number:
            phase(number - 1)
        accumulate(all_images, all_texts, strip_i, top_c, sum_c, low, high)
        accumulate(all_texts, all_images, strip_t, top_r, sum_r, low, high)

    row_lse = top_r[...] + jnp.log(sum_r[...])
    col_lse = top_c[...] + jnp.log(sum_c[...])
    own_r, own_c = row_lse[:, 0:rows], col_lse[:, 0:rows]
    cot_r, cot_c = cot_ref[0:1, :], cot_ref[1:2, :]
    own_r_col, own_c_col = as_column(own_r, rows), as_column(own_c, rows)
    cot_r_col, cot_c_col = as_column(cot_r, rows), as_column(cot_c, rows)
    count = all_cot.shape[0]
    for slot in range(count):
        r_row = cot_r if slot == 0 else all_cot[slot, 0:1, :]
        c_row = cot_c if slot == 0 else all_cot[slot, 1:2, :]
        for at in range(0, rows, LANES):
            span = slice(slot * rows + at, slot * rows + at + LANES)
            part_i, part_t = strip_i[:, span], strip_t[:, span]
            weights_i[:, span] = (
                cot_r_col * jnp.exp(part_i - own_r_col)
                + c_row[:, at : at + LANES] * jnp.exp(part_i - col_lse[:, span])
            ).astype(jnp.bfloat16)
            weights_t[:, span] = (
                r_row[:, at : at + LANES] * jnp.exp(part_t - row_lse[:, span])
                + cot_c_col * jnp.exp(part_t - own_c_col)
            ).astype(jnp.bfloat16)

    both_cot = cot_r_col + cot_c_col
    product = jnp.zeros((rows, LANES), jnp.float32)
    terms_i = jnp.dot(weights_i[...], all_texts[...], preferred_element_type=jnp.float32)
    terms_t = jnp.dot(weights_t[...], all_images[...], preferred_element_type=jnp.float32)
    for at in range(0, width, LANES):
        span = slice(at, at + LANES)
        image = images_ref[:, span].astype(jnp.float32)
        text = texts_ref[:, span].astype(jnp.float32)
        product = product + image * text
        grad_images_ref[:, span] = scale * (terms_i[:, span] - both_cot * text)
        grad_texts_ref[:, span] = scale * (terms_t[:, span] - both_cot * image)
    matched = scale * jnp.sum(jnp.transpose(product), axis=0, keepdims=True)
    losses_ref[0:1, :] = own_r - matched
    losses_ref[1:2, :] = own_c - matched

    for half in range(LINE // 2):

        @pl.when(from_end == half)
        def _():
            for one in sent[half]:
                copy(*one).wait_send()


def exchange(images, texts, scale, cotangent, count):
    rows, width = images.shape
    total = count * rows
    vmem = pl.BlockSpec(memory_space=pltpu.VMEM)
    return pl.pallas_call(
        kernel,
        out_shape=(
            jax.ShapeDtypeStruct((2, rows), jnp.float32),
            jax.ShapeDtypeStruct((rows, width), jnp.float32),
            jax.ShapeDtypeStruct((rows, width), jnp.float32),
        ),
        in_specs=[pl.BlockSpec(memory_space=pltpu.SMEM), vmem, vmem, vmem],
        out_specs=(vmem, vmem, vmem),
        scratch_shapes=[
            pltpu.VMEM((total, width), jnp.bfloat16),
            pltpu.VMEM((total, width), jnp.bfloat16),
            pltpu.VMEM((count, 2, rows), jnp.float32),
            pltpu.VMEM((rows, total), jnp.float32),
            pltpu.VMEM((rows, total), jnp.float32),
            pltpu.VMEM((1, total), jnp.float32),
            pltpu.VMEM((1, total), jnp.float32),
            pltpu.VMEM((1, total), jnp.float32),
            pltpu.VMEM((1, total), jnp.float32),
            pltpu.VMEM((rows, total), jnp.bfloat16),
            pltpu.VMEM((rows, total), jnp.bfloat16),
            pltpu.SemaphoreType.DMA((3, count, 3)),
            pltpu.SemaphoreType.DMA((3, count)),
        ],
        compiler_params=pltpu.CompilerParams(collective_id=0, has_side_effects=True),
    )(scale, images, texts, cotangent)


def dot_rows(left, right):
    return lax.dot_general(
        left, right, (((1,), (1,)), ((), ())), preferred_element_type=jnp.float32
    )


def dot_lead(left, right):
    return lax.dot_general(
        left, right, (((0,), (0,)), ((), ())), preferred_element_type=jnp.float32
    )


def merge_pair(first, second):
    max_new = jnp.maximum(first[0], second[0])
    return (
        max_new,
        first[1] * jnp.exp(first[0] - max_new) + second[1] * jnp.exp(second[0] - max_new),
    )


def block_stats(scores, along):
    top_value = jnp.max(scores, axis=along)
    total_sum = jnp.sum(jnp.exp(scores - jnp.expand_dims(top_value, along)), axis=along)
    return (top_value, total_sum)


def shards(images, texts, scale, cotangent):
    row_count = images.shape[0]
    logit_scale = scale[0]
    cot_rows = cotangent[0]
    cot_cols = cotangent[1]
    low_start = jnp.full((row_count,), -1e30, jnp.float32)
    zero_sums = jnp.zeros((row_count,), jnp.float32)
    all_images, all_texts = (
        lax.all_gather(images, "blk", axis=0, tiled=True),
        lax.all_gather(texts, "blk", axis=0, tiled=True),
    )
    batch_total = all_images.shape[0]
    block_width = min(batch_total, 1024)
    block_count = batch_total // block_width

    def first_pass(step, carried):
        row_part, col_part = carried
        text_block = lax.dynamic_slice_in_dim(all_texts, step * block_width, block_width, 0)
        image_block = lax.dynamic_slice_in_dim(all_images, step * block_width, block_width, 0)
        row_scores = logit_scale * dot_rows(text_block, images)
        col_scores = logit_scale * dot_rows(image_block, texts)
        return (
            merge_pair(row_part, block_stats(row_scores, 0)),
            merge_pair(col_part, block_stats(col_scores, 0)),
        )

    row_part, col_part = lax.fori_loop(
        0, block_count, first_pass, ((low_start, zero_sums), (low_start, zero_sums))
    )
    row_lse = row_part[0] + jnp.log(row_part[1])
    col_lse = col_part[0] + jnp.log(col_part[1])
    matched = logit_scale * jnp.sum(images.astype(jnp.float32) * texts.astype(jnp.float32), axis=1)
    row_losses = jnp.stack([row_lse - matched, col_lse - matched])
    all_row_lse, all_col_lse, all_cot_rows, all_cot_cols = (
        lax.all_gather(row_lse, "blk", axis=0, tiled=True),
        lax.all_gather(col_lse, "blk", axis=0, tiled=True),
        lax.all_gather(cot_rows, "blk", axis=0, tiled=True),
        lax.all_gather(cot_cols, "blk", axis=0, tiled=True),
    )

    def second_pass(step, carried):
        acc_images, acc_texts = carried
        start = step * block_width
        text_block = lax.dynamic_slice_in_dim(all_texts, start, block_width, 0)
        image_block = lax.dynamic_slice_in_dim(all_images, start, block_width, 0)
        col_lse_block = lax.dynamic_slice_in_dim(all_col_lse, start, block_width, 0)
        col_cot_block = lax.dynamic_slice_in_dim(all_cot_cols, start, block_width, 0)
        row_lse_block = lax.dynamic_slice_in_dim(all_row_lse, start, block_width, 0)
        row_cot_block = lax.dynamic_slice_in_dim(all_cot_rows, start, block_width, 0)
        row_scores = logit_scale * dot_rows(text_block, images)
        row_weights = cot_rows[None, :] * jnp.exp(row_scores - row_lse[None, :]) + col_cot_block[
            :, None
        ] * jnp.exp(row_scores - col_lse_block[:, None])
        acc_images = acc_images + dot_lead(row_weights.astype(jnp.bfloat16), text_block)
        col_scores = logit_scale * dot_rows(image_block, texts)
        col_weights = row_cot_block[:, None] * jnp.exp(
            col_scores - row_lse_block[:, None]
        ) + cot_cols[None, :] * jnp.exp(col_scores - col_lse[None, :])
        acc_texts = acc_texts + dot_lead(col_weights.astype(jnp.bfloat16), image_block)
        return (acc_images, acc_texts)

    zero_grads = jnp.zeros((row_count, images.shape[1]), jnp.float32)
    image_terms, text_terms = lax.fori_loop(0, block_count, second_pass, (zero_grads, zero_grads))
    both_cot = (cot_rows + cot_cols)[:, None]
    grad_images = logit_scale * (image_terms - both_cot * texts.astype(jnp.float32))
    grad_texts = logit_scale * (text_terms - both_cot * images.astype(jnp.float32))
    return (row_losses, grad_images, grad_texts)


def solution(mesh):
    count = mesh.shape["blk"]

    def step(images, texts, scale, cotangent):
        if count == 2 * LINE and images.shape[0] % LANES == 0:
            return exchange(images, texts, scale, cotangent, count)
        return shards(images, texts, scale, cotangent)

    return jax.shard_map(
        step,
        mesh=mesh,
        in_specs=(P(("dp", "blk"), None), P(("dp", "blk"), None), P(), P(None, ("dp", "blk"))),
        out_specs=(P(None, ("dp", "blk")), P(("dp", "blk"), None), P(("dp", "blk"), None)),
        check_vma=False,
    )
```

```python
import jax
import jax.numpy as jnp
from jax import lax
from jax.experimental import pallas as pl
from jax.experimental.pallas import tpu as pltpu
from jax.sharding import PartitionSpec as P

LANES = 128
VMEM_BYTES = 67043328
MARGIN = 4096
MESH = pl.DeviceIdType.MESH

SLOTS = (
    ((0, 0), (0, 1), (1, 0), (1, 1), (2, 0), (2, 1), (3, 0), (3, 1)),
    ((1, 0), (1, 1), (0, 0), (2, 0), (0, 1), (3, 0), (2, 1), (3, 1)),
)
LINE = len(SLOTS[0]) // 2
PHASES = (
    (
        [
            ("I", (0, 1), "i"), ("I", (1, 0), "x"), ("T", (0, 1), "i"), ("T", (1, 0), "x"),
        ],
        [("I", (1, 1), ""), ("I", (2, 0), "x"), ("T", (1, 1), ""), ("T", (2, 0), "x")],
        [("I", (2, 1), ""), ("I", (3, 0), "x"), ("T", (2, 1), ""), ("T", (3, 0), "")],
        [("I", (3, 1), ""), ("T", (3, 1), "")],
    ),
    (
        [
            ("I", (1, 1), ""), ("I", (0, 0), "i"), ("I", (2, 0), "ox"),
            ("T", (1, 1), ""), ("T", (0, 0), "i"), ("T", (2, 0), "ox"),
        ],
        [
            ("I", (0, 1), ""), ("I", (3, 0), "o"), ("T", (0, 1), ""),
            ("T", (3, 0), "ox"), ("I", (3, 0), "X"),
        ],
        [("I", (2, 1), ""), ("T", (2, 1), "")],
        [("T", (3, 1), "o"), ("I", (3, 1), "")],
    ),
)
GROUPS = ((0, 1), (1, 3), (3, 5), (5, 7), (7, 8))
OWN_WAYS = ("ix", "iox")


def landing(half, block, way):
    place, other = block
    if way == "x":
        return half, (place, 1 - other)
    if way == "o":
        return half - 1, block
    if half == LINE // 2 - 1:
        return half, (LINE - 1 - place, other)
    return half + 1, block


def as_column(row, rows):
    return jnp.transpose(jnp.broadcast_to(row, (LANES, rows)))


def fold(top_ref, sum_ref, tile, low, high, fresh):
    top = jnp.max(tile, axis=0, keepdims=True)
    if fresh:
        sum_ref[:, low:high] = jnp.sum(jnp.exp(tile - top), axis=0, keepdims=True)
    else:
        before = top_ref[:, low:high]
        top = jnp.maximum(before, top)
        sum_ref[:, low:high] = sum_ref[:, low:high] * jnp.exp(before - top) + jnp.sum(
            jnp.exp(tile - top), axis=0, keepdims=True
        )
    top_ref[:, low:high] = top


def kernel(
    scale_ref, images_ref, texts_ref, cot_ref,
    all_images, all_texts, all_cot, weights_i, weights_t, lses_ref,
    strip_i, strip_t, top_r, sum_r, top_c, sum_c, send_sem, recv_sem, own_sem,
):
    rows, width = images_ref.shape
    me = lax.axis_index("blk")
    place, column = me // 2, lax.rem(me, 2)
    upper = place // (LINE // 2)
    step = 1 - 2 * upper
    from_end = place + upper * (LINE - 1 - 2 * place)
    peers = {
        "x": place * 2 + 1 - column,
        "i": (place + step) * 2 + column,
        "o": (place - step) * 2 + column,
    }
    kinds = "ITC"

    def part(kind, slot):
        if kind == "C":
            return all_cot.at[slot]
        return (all_images if kind == "I" else all_texts).at[pl.ds(slot * rows, rows)]

    def copy(half, kind, block, way):
        slot = SLOTS[half].index(block)
        there, name = landing(half, block, way)
        own = {"I": images_ref, "T": texts_ref, "C": cot_ref}[kind]
        target = SLOTS[there].index(name)
        at = kinds.index(kind)
        return pltpu.make_async_remote_copy(
            src_ref=own if slot == 0 else part(kind, slot),
            dst_ref=part(kind, target),
            send_sem=send_sem.at[at, slot, "xio".index(way)],
            recv_sem=recv_sem.at[at, target],
            device_id={"blk": peers[way]},
            device_id_type=MESH,
        )

    def arrived(half, kind, block):
        slot = SLOTS[half].index(block)
        at = kinds.index(kind)
        pltpu.make_async_remote_copy(
            src_ref=part(kind, slot),
            dst_ref=part(kind, slot),
            send_sem=send_sem.at[at, slot, 0],
            recv_sem=recv_sem.at[at, slot],
            device_id={"blk": peers["x"]},
            device_id_type=MESH,
        ).wait_recv()

    def both(kind):
        return ("C", "T") if kind == "T" else ("I",)

    sent = ([], [])

    def phase(number):
        for half in range(LINE // 2):

            @pl.when(from_end == half)
            def _():
                for kind, block, ways in PHASES[half][number]:
                    for each in both(kind):
                        if ways != "X":
                            arrived(half, each, block)
                        for way in ways.lower():
                            one = (half, each, block, way)
                            copy(*one).start()
                            sent[half].append(one)

    mine = [
        pltpu.make_async_copy(source, part(kind, 0), own_sem.at[kinds.index(kind)])
        for kind, source in zip(kinds, (images_ref, texts_ref, cot_ref))
    ]
    barrier = pltpu.get_barrier_semaphore()
    for half in range(LINE // 2):

        @pl.when(from_end == half)
        def _():
            for way in OWN_WAYS[half]:
                pl.semaphore_signal(barrier, inc=1, device_id={"blk": peers[way]}, device_id_type=MESH)
            pl.semaphore_wait(barrier, len(OWN_WAYS[half]))
            for kind in "ICT":
                for way in OWN_WAYS[half]:
                    one = (half, kind, SLOTS[half][0], way)
                    copy(*one).start()
                    sent[half].append(one)

    scale = scale_ref[0]
    for each in mine:
        each.start()
    for each in mine:
        each.wait()

    def scores(left, right):
        return scale * dot_rows(left, right)

    def accumulate(left, right, strip, top, total, low, high):
        old, new = low * rows, high * rows
        tile = scores(left[old:new, :], right[0:new, :])
        fold(top, total, tile[:, old:], old, new, True)
        if low == 0:
            strip[:, old:new] = tile
            return
        fold(top, total, tile[:, :old], 0, old, False)
        tile = scores(left[0:old, :], right[old:new, :])
        strip[:, old:new] = tile[0:rows, :]
        fold(top, total, tile, old, new, False)

    for number, (low, high) in enumerate(GROUPS):
        if number:
            phase(number - 1)
        accumulate(all_images, all_texts, strip_i, top_c, sum_c, low, high)
        accumulate(all_texts, all_images, strip_t, top_r, sum_r, low, high)

    row_lse = top_r[...] + jnp.log(sum_r[...])
    col_lse = top_c[...] + jnp.log(sum_c[...])
    own_r, own_c = row_lse[:, 0:rows], col_lse[:, 0:rows]
    lses_ref[0:1, :] = own_r
    lses_ref[1:2, :] = own_c
    cot_r, cot_c = all_cot[0, 0:1, :], all_cot[0, 1:2, :]
    own_r_col, own_c_col = as_column(own_r, rows), as_column(own_c, rows)
    cot_r_col, cot_c_col = as_column(cot_r, rows), as_column(cot_c, rows)
    count = all_cot.shape[0]
    for slot in range(count):
        r_row, c_row = all_cot[slot, 0:1, :], all_cot[slot, 1:2, :]
        for at in range(0, rows, LANES):
            span = slice(slot * rows + at, slot * rows + at + LANES)
            part_i, part_t = strip_i[:, span], strip_t[:, span]
            weights_i[:, span] = (
                cot_r_col * jnp.exp(part_i - own_r_col)
                + c_row[:, at : at + LANES] * jnp.exp(part_i - col_lse[:, span])
            ).astype(jnp.bfloat16)
            weights_t[:, span] = (
                r_row[:, at : at + LANES] * jnp.exp(part_t - row_lse[:, span])
                + cot_c_col * jnp.exp(part_t - own_c_col)
            ).astype(jnp.bfloat16)

    for half in range(LINE // 2):

        @pl.when(from_end == half)
        def _():
            for one in sent[half]:
                copy(*one).wait_send()


def finish(
    scale_ref, all_images, all_texts, all_cot, weights_i, weights_t, lses_ref,
    losses_ref, grad_images_ref, grad_texts_ref, losses, grad_images, grad_texts, sem,
):
    rows, width = grad_images.shape
    scale = scale_ref[0]
    both_cot = as_column(all_cot[0, 0:1, :] + all_cot[0, 1:2, :], rows)
    outs = [
        pltpu.make_async_copy(*pair, sem.at[at])
        for at, pair in enumerate(
            ((grad_images, grad_images_ref), (grad_texts, grad_texts_ref), (losses, losses_ref))
        )
    ]
    terms = jnp.dot(weights_i[...], all_texts[...], preferred_element_type=jnp.float32)
    product = jnp.zeros((rows, LANES), jnp.float32)
    for at in range(0, width, LANES):
        span = slice(at, at + LANES)
        text = all_texts[0:rows, span].astype(jnp.float32)
        product = product + all_images[0:rows, span].astype(jnp.float32) * text
        grad_images[:, span] = scale * (terms[:, span] - both_cot * text)
    outs[0].start()
    matched = scale * jnp.sum(jnp.transpose(product), axis=0, keepdims=True)
    losses[...] = lses_ref[...] - matched
    outs[2].start()
    terms = jnp.dot(weights_t[...], all_images[...], preferred_element_type=jnp.float32)
    for at in range(0, width, LANES):
        span = slice(at, at + LANES)
        image = all_images[0:rows, span].astype(jnp.float32)
        grad_texts[:, span] = scale * (terms[:, span] - both_cot * image)
    outs[1].start()
    for out in outs:
        out.wait()


def exchange(images, texts, scale, cotangent, count):
    rows, width = images.shape
    total = count * rows
    vmem = pl.BlockSpec(memory_space=pltpu.VMEM)
    smem = pl.BlockSpec(memory_space=pltpu.SMEM)
    hbm = pl.BlockSpec(memory_space=pltpu.HBM)
    f32, bf16 = jnp.float32, jnp.bfloat16
    kept = (
        pltpu.VMEM((total, width), bf16),
        pltpu.VMEM((total, width), bf16),
        pltpu.VMEM((count, 2, rows), f32),
        pltpu.VMEM((rows, total), bf16),
        pltpu.VMEM((rows, total), bf16),
        pltpu.VMEM((2, rows), f32),
    )
    handed_on = 2 * total * (2 * width + 2 * rows) + 4 * 2 * rows * (count + 1)
    grant = VMEM_BYTES - handed_on - MARGIN
    gathered = pl.pallas_call(
        kernel,
        out_shape=kept,
        in_specs=[smem, hbm, hbm, hbm],
        out_specs=(vmem,) * len(kept),
        scratch_shapes=[
            pltpu.VMEM((rows, total), f32),
            pltpu.VMEM((rows, total), f32),
            pltpu.VMEM((1, total), f32),
            pltpu.VMEM((1, total), f32),
            pltpu.VMEM((1, total), f32),
            pltpu.VMEM((1, total), f32),
            pltpu.SemaphoreType.DMA((3, count, 3)),
            pltpu.SemaphoreType.DMA((3, count)),
            pltpu.SemaphoreType.DMA((3,)),
        ],
        compiler_params=pltpu.CompilerParams(
            collective_id=0, has_side_effects=True, vmem_limit_bytes=grant
        ),
    )(scale, images, texts, cotangent)
    outs = (
        jax.ShapeDtypeStruct((2, rows), f32),
        jax.ShapeDtypeStruct((rows, width), f32),
        jax.ShapeDtypeStruct((rows, width), f32),
    )
    return pl.pallas_call(
        finish,
        out_shape=outs,
        in_specs=[smem] + [vmem] * len(kept),
        out_specs=(hbm,) * len(outs),
        scratch_shapes=[pltpu.VMEM(out.shape, f32) for out in outs] + [pltpu.SemaphoreType.DMA((3,))],
        compiler_params=pltpu.CompilerParams(vmem_limit_bytes=grant // 2),
    )(scale, *gathered)


def dot_rows(left, right):
    return lax.dot_general(
        left, right, (((1,), (1,)), ((), ())), preferred_element_type=jnp.float32
    )


def dot_lead(left, right):
    return lax.dot_general(
        left, right, (((0,), (0,)), ((), ())), preferred_element_type=jnp.float32
    )


def merge_pair(first, second):
    max_new = jnp.maximum(first[0], second[0])
    return (
        max_new,
        first[1] * jnp.exp(first[0] - max_new) + second[1] * jnp.exp(second[0] - max_new),
    )


def block_stats(scores, along):
    top_value = jnp.max(scores, axis=along)
    total_sum = jnp.sum(jnp.exp(scores - jnp.expand_dims(top_value, along)), axis=along)
    return (top_value, total_sum)


def shards(images, texts, scale, cotangent):
    row_count = images.shape[0]
    logit_scale = scale[0]
    cot_rows = cotangent[0]
    cot_cols = cotangent[1]
    low_start = jnp.full((row_count,), -1e30, jnp.float32)
    zero_sums = jnp.zeros((row_count,), jnp.float32)
    all_images, all_texts = (
        lax.all_gather(images, "blk", axis=0, tiled=True),
        lax.all_gather(texts, "blk", axis=0, tiled=True),
    )
    batch_total = all_images.shape[0]
    block_width = min(batch_total, 1024)
    block_count = batch_total // block_width

    def first_pass(step, carried):
        row_part, col_part = carried
        text_block = lax.dynamic_slice_in_dim(all_texts, step * block_width, block_width, 0)
        image_block = lax.dynamic_slice_in_dim(all_images, step * block_width, block_width, 0)
        row_scores = logit_scale * dot_rows(text_block, images)
        col_scores = logit_scale * dot_rows(image_block, texts)
        return (
            merge_pair(row_part, block_stats(row_scores, 0)),
            merge_pair(col_part, block_stats(col_scores, 0)),
        )

    row_part, col_part = lax.fori_loop(
        0, block_count, first_pass, ((low_start, zero_sums), (low_start, zero_sums))
    )
    row_lse = row_part[0] + jnp.log(row_part[1])
    col_lse = col_part[0] + jnp.log(col_part[1])
    matched = logit_scale * jnp.sum(images.astype(jnp.float32) * texts.astype(jnp.float32), axis=1)
    row_losses = jnp.stack([row_lse - matched, col_lse - matched])
    all_row_lse, all_col_lse, all_cot_rows, all_cot_cols = (
        lax.all_gather(row_lse, "blk", axis=0, tiled=True),
        lax.all_gather(col_lse, "blk", axis=0, tiled=True),
        lax.all_gather(cot_rows, "blk", axis=0, tiled=True),
        lax.all_gather(cot_cols, "blk", axis=0, tiled=True),
    )

    def second_pass(step, carried):
        acc_images, acc_texts = carried
        start = step * block_width
        text_block = lax.dynamic_slice_in_dim(all_texts, start, block_width, 0)
        image_block = lax.dynamic_slice_in_dim(all_images, start, block_width, 0)
        col_lse_block = lax.dynamic_slice_in_dim(all_col_lse, start, block_width, 0)
        col_cot_block = lax.dynamic_slice_in_dim(all_cot_cols, start, block_width, 0)
        row_lse_block = lax.dynamic_slice_in_dim(all_row_lse, start, block_width, 0)
        row_cot_block = lax.dynamic_slice_in_dim(all_cot_rows, start, block_width, 0)
        row_scores = logit_scale * dot_rows(text_block, images)
        row_weights = cot_rows[None, :] * jnp.exp(row_scores - row_lse[None, :]) + col_cot_block[
            :, None
        ] * jnp.exp(row_scores - col_lse_block[:, None])
        acc_images = acc_images + dot_lead(row_weights.astype(jnp.bfloat16), text_block)
        col_scores = logit_scale * dot_rows(image_block, texts)
        col_weights = row_cot_block[:, None] * jnp.exp(
            col_scores - row_lse_block[:, None]
        ) + cot_cols[None, :] * jnp.exp(col_scores - col_lse[None, :])
        acc_texts = acc_texts + dot_lead(col_weights.astype(jnp.bfloat16), image_block)
        return (acc_images, acc_texts)

    zero_grads = jnp.zeros((row_count, images.shape[1]), jnp.float32)
    image_terms, text_terms = lax.fori_loop(0, block_count, second_pass, (zero_grads, zero_grads))
    both_cot = (cot_rows + cot_cols)[:, None]
    grad_images = logit_scale * (image_terms - both_cot * texts.astype(jnp.float32))
    grad_texts = logit_scale * (text_terms - both_cot * images.astype(jnp.float32))
    return (row_losses, grad_images, grad_texts)


def solution(mesh):
    count = mesh.shape["blk"]

    def step(images, texts, scale, cotangent):
        if count == 2 * LINE and images.shape[0] % LANES == 0:
            return exchange(images, texts, scale, cotangent, count)
        return shards(images, texts, scale, cotangent)

    return jax.shard_map(
        step,
        mesh=mesh,
        in_specs=(P(("dp", "blk"), None), P(("dp", "blk"), None), P(), P(None, ("dp", "blk"))),
        out_specs=(P(None, ("dp", "blk")), P(("dp", "blk"), None), P(("dp", "blk"), None)),
        check_vma=False,
    )
```

```python
import jax
import jax.numpy as jnp
from jax import lax
from jax.experimental import pallas as pl
from jax.experimental.pallas import tpu as pltpu
from jax.sharding import PartitionSpec as P

LANES = 128
VMEM_BYTES = 67043328
MARGIN = 4096
MESH = pl.DeviceIdType.MESH

SLOTS = (
    ((0, 0), (0, 1), (1, 0), (1, 1), (2, 0), (2, 1), (3, 0), (3, 1)),
    ((1, 0), (1, 1), (0, 0), (2, 0), (0, 1), (3, 0), (2, 1), (3, 1)),
)
LINE = len(SLOTS[0]) // 2
PHASES = (
    (
        [
            ("I", (0, 1), "i"), ("I", (1, 0), "x"), ("T", (0, 1), "i"), ("T", (1, 0), "x"),
        ],
        [("I", (1, 1), ""), ("I", (2, 0), "x"), ("T", (1, 1), ""), ("T", (2, 0), "x")],
        [("I", (2, 1), ""), ("I", (3, 0), "x"), ("T", (2, 1), ""), ("T", (3, 0), "")],
        [("I", (3, 1), ""), ("T", (3, 1), "")],
    ),
    (
        [
            ("I", (1, 1), ""), ("I", (0, 0), "i"), ("I", (2, 0), "ox"),
            ("T", (1, 1), ""), ("T", (0, 0), "i"), ("T", (2, 0), "ox"),
        ],
        [
            ("I", (0, 1), ""), ("I", (3, 0), "o"), ("T", (0, 1), ""),
            ("T", (3, 0), "ox"), ("I", (3, 0), "X"),
        ],
        [("I", (2, 1), ""), ("T", (2, 1), ""), ("T", (3, 1), "o")],
        [("I", (3, 1), "")],
    ),
)
GROUPS = ((0, 1), (1, 3), (3, 5), (5, 7), (7, 8))
OWN_WAYS = ("ix", "iox")


def landing(half, block, way):
    place, other = block
    if way == "x":
        return half, (place, 1 - other)
    if way == "o":
        return half - 1, block
    if half == LINE // 2 - 1:
        return half, (LINE - 1 - place, other)
    return half + 1, block


def as_column(row, rows):
    return jnp.transpose(jnp.broadcast_to(row, (LANES, rows)))


def fold(top_ref, sum_ref, tile, low, high, fresh):
    top = jnp.max(tile, axis=0, keepdims=True)
    if fresh:
        sum_ref[:, low:high] = jnp.sum(jnp.exp(tile - top), axis=0, keepdims=True)
    else:
        before = top_ref[:, low:high]
        top = jnp.maximum(before, top)
        sum_ref[:, low:high] = sum_ref[:, low:high] * jnp.exp(before - top) + jnp.sum(
            jnp.exp(tile - top), axis=0, keepdims=True
        )
    top_ref[:, low:high] = top


def kernel(
    scale_ref, images_ref, texts_ref, cot_ref,
    all_images, all_texts, all_cot, weights_i, weights_t, lses_ref,
    strip_i, strip_t, top_r, sum_r, top_c, sum_c, send_sem, recv_sem, own_sem,
):
    rows, width = images_ref.shape
    me = lax.axis_index("blk")
    place, column = me // 2, lax.rem(me, 2)
    upper = place // (LINE // 2)
    step = 1 - 2 * upper
    from_end = place + upper * (LINE - 1 - 2 * place)
    peers = {
        "x": place * 2 + 1 - column,
        "i": (place + step) * 2 + column,
        "o": (place - step) * 2 + column,
    }
    kinds = "ITC"

    def part(kind, slot):
        if kind == "C":
            return all_cot.at[slot]
        return (all_images if kind == "I" else all_texts).at[pl.ds(slot * rows, rows)]

    def copy(half, kind, block, way):
        slot = SLOTS[half].index(block)
        there, name = landing(half, block, way)
        own = {"I": images_ref, "T": texts_ref, "C": cot_ref}[kind]
        target = SLOTS[there].index(name)
        at = kinds.index(kind)
        return pltpu.make_async_remote_copy(
            src_ref=own if slot == 0 else part(kind, slot),
            dst_ref=part(kind, target),
            send_sem=send_sem.at[at, slot, "xio".index(way)],
            recv_sem=recv_sem.at[at, target],
            device_id={"blk": peers[way]},
            device_id_type=MESH,
        )

    def arrived(half, kind, block):
        slot = SLOTS[half].index(block)
        at = kinds.index(kind)
        pltpu.make_async_remote_copy(
            src_ref=part(kind, slot),
            dst_ref=part(kind, slot),
            send_sem=send_sem.at[at, slot, 0],
            recv_sem=recv_sem.at[at, slot],
            device_id={"blk": peers["x"]},
            device_id_type=MESH,
        ).wait_recv()

    def both(kind):
        return ("C", "T") if kind == "T" else ("I",)

    sent = ([], [])

    def phase(number):
        for half in range(LINE // 2):

            @pl.when(from_end == half)
            def _():
                for kind, block, ways in PHASES[half][number]:
                    for each in both(kind):
                        if ways != "X":
                            arrived(half, each, block)
                        for way in ways.lower():
                            one = (half, each, block, way)
                            copy(*one).start()
                            sent[half].append(one)

    mine = [
        pltpu.make_async_copy(source, part(kind, 0), own_sem.at[kinds.index(kind)])
        for kind, source in zip(kinds, (images_ref, texts_ref, cot_ref))
    ]
    barrier = pltpu.get_barrier_semaphore()
    for half in range(LINE // 2):

        @pl.when(from_end == half)
        def _():
            for way in OWN_WAYS[half]:
                pl.semaphore_signal(barrier, inc=1, device_id={"blk": peers[way]}, device_id_type=MESH)
            pl.semaphore_wait(barrier, len(OWN_WAYS[half]))
            for kind in "ICT":
                for way in OWN_WAYS[half]:
                    one = (half, kind, SLOTS[half][0], way)
                    copy(*one).start()
                    sent[half].append(one)

    scale = scale_ref[0]
    for each in mine:
        each.start()
    for each in mine:
        each.wait()

    def scores(left, right):
        return scale * dot_rows(left, right)

    def accumulate(left, right, strip, top, total, low, high):
        old, new = low * rows, high * rows
        tile = scores(left[old:new, :], right[0:new, :])
        fold(top, total, tile[:, old:], old, new, True)
        if low == 0:
            strip[:, old:new] = tile
            return
        fold(top, total, tile[:, :old], 0, old, False)
        tile = scores(left[0:old, :], right[old:new, :])
        strip[:, old:new] = tile[0:rows, :]
        fold(top, total, tile, old, new, False)

    for number, (low, high) in enumerate(GROUPS):
        if number:
            phase(number - 1)
        accumulate(all_images, all_texts, strip_i, top_c, sum_c, low, high)
        accumulate(all_texts, all_images, strip_t, top_r, sum_r, low, high)

    row_lse = top_r[...] + jnp.log(sum_r[...])
    col_lse = top_c[...] + jnp.log(sum_c[...])
    own_r, own_c = row_lse[:, 0:rows], col_lse[:, 0:rows]
    lses_ref[0:1, :] = own_r
    lses_ref[1:2, :] = own_c
    cot_r, cot_c = all_cot[0, 0:1, :], all_cot[0, 1:2, :]
    own_r_col, own_c_col = as_column(own_r, rows), as_column(own_c, rows)
    cot_r_col, cot_c_col = as_column(cot_r, rows), as_column(cot_c, rows)
    count = all_cot.shape[0]
    for slot in range(count):
        r_row, c_row = all_cot[slot, 0:1, :], all_cot[slot, 1:2, :]
        for at in range(0, rows, LANES):
            span = slice(slot * rows + at, slot * rows + at + LANES)
            part_i, part_t = strip_i[:, span], strip_t[:, span]
            weights_i[:, span] = (
                cot_r_col * jnp.exp(part_i - own_r_col)
                + c_row[:, at : at + LANES] * jnp.exp(part_i - col_lse[:, span])
            ).astype(jnp.bfloat16)
            weights_t[:, span] = (
                r_row[:, at : at + LANES] * jnp.exp(part_t - row_lse[:, span])
                + cot_c_col * jnp.exp(part_t - own_c_col)
            ).astype(jnp.bfloat16)

    for half in range(LINE // 2):

        @pl.when(from_end == half)
        def _():
            for one in sent[half]:
                copy(*one).wait_send()


def finish(
    scale_ref, all_images, all_texts, all_cot, weights_i, weights_t, lses_ref,
    losses_ref, grad_images_ref, grad_texts_ref, losses, grad_images, grad_texts, sem,
):
    rows, width = grad_images.shape
    scale = scale_ref[0]
    both_cot = as_column(all_cot[0, 0:1, :] + all_cot[0, 1:2, :], rows)
    outs = [
        pltpu.make_async_copy(*pair, sem.at[at])
        for at, pair in enumerate(
            ((grad_images, grad_images_ref), (grad_texts, grad_texts_ref), (losses, losses_ref))
        )
    ]
    terms = jnp.dot(weights_i[...], all_texts[...], preferred_element_type=jnp.float32)
    product = jnp.zeros((rows, LANES), jnp.float32)
    for at in range(0, width, LANES):
        span = slice(at, at + LANES)
        text = all_texts[0:rows, span].astype(jnp.float32)
        product = product + all_images[0:rows, span].astype(jnp.float32) * text
        grad_images[:, span] = scale * (terms[:, span] - both_cot * text)
    outs[0].start()
    matched = scale * jnp.sum(jnp.transpose(product), axis=0, keepdims=True)
    losses[...] = lses_ref[...] - matched
    outs[2].start()
    terms = jnp.dot(weights_t[...], all_images[...], preferred_element_type=jnp.float32)
    for at in range(0, width, LANES):
        span = slice(at, at + LANES)
        image = all_images[0:rows, span].astype(jnp.float32)
        grad_texts[:, span] = scale * (terms[:, span] - both_cot * image)
    outs[1].start()
    for out in outs:
        out.wait()


def exchange(images, texts, scale, cotangent, count):
    rows, width = images.shape
    total = count * rows
    vmem = pl.BlockSpec(memory_space=pltpu.VMEM)
    smem = pl.BlockSpec(memory_space=pltpu.SMEM)
    hbm = pl.BlockSpec(memory_space=pltpu.HBM)
    f32, bf16 = jnp.float32, jnp.bfloat16
    kept = (
        pltpu.VMEM((total, width), bf16),
        pltpu.VMEM((total, width), bf16),
        pltpu.VMEM((count, 2, rows), f32),
        pltpu.VMEM((rows, total), bf16),
        pltpu.VMEM((rows, total), bf16),
        pltpu.VMEM((2, rows), f32),
    )
    handed_on = 2 * total * (2 * width + 2 * rows) + 4 * 2 * rows * (count + 1)
    grant = VMEM_BYTES - handed_on - MARGIN
    gathered = pl.pallas_call(
        kernel,
        out_shape=kept,
        in_specs=[smem, hbm, hbm, hbm],
        out_specs=(vmem,) * len(kept),
        scratch_shapes=[
            pltpu.VMEM((rows, total), f32),
            pltpu.VMEM((rows, total), f32),
            pltpu.VMEM((1, total), f32),
            pltpu.VMEM((1, total), f32),
            pltpu.VMEM((1, total), f32),
            pltpu.VMEM((1, total), f32),
            pltpu.SemaphoreType.DMA((3, count, 3)),
            pltpu.SemaphoreType.DMA((3, count)),
            pltpu.SemaphoreType.DMA((3,)),
        ],
        compiler_params=pltpu.CompilerParams(
            collective_id=0, has_side_effects=True, vmem_limit_bytes=grant
        ),
    )(scale, images, texts, cotangent)
    outs = (
        jax.ShapeDtypeStruct((2, rows), f32),
        jax.ShapeDtypeStruct((rows, width), f32),
        jax.ShapeDtypeStruct((rows, width), f32),
    )
    return pl.pallas_call(
        finish,
        out_shape=outs,
        in_specs=[smem] + [vmem] * len(kept),
        out_specs=(hbm,) * len(outs),
        scratch_shapes=[pltpu.VMEM(out.shape, f32) for out in outs] + [pltpu.SemaphoreType.DMA((3,))],
        compiler_params=pltpu.CompilerParams(vmem_limit_bytes=grant // 2),
    )(scale, *gathered)


def dot_rows(left, right):
    return lax.dot_general(
        left, right, (((1,), (1,)), ((), ())), preferred_element_type=jnp.float32
    )


def dot_lead(left, right):
    return lax.dot_general(
        left, right, (((0,), (0,)), ((), ())), preferred_element_type=jnp.float32
    )


def merge_pair(first, second):
    max_new = jnp.maximum(first[0], second[0])
    return (
        max_new,
        first[1] * jnp.exp(first[0] - max_new) + second[1] * jnp.exp(second[0] - max_new),
    )


def block_stats(scores, along):
    top_value = jnp.max(scores, axis=along)
    total_sum = jnp.sum(jnp.exp(scores - jnp.expand_dims(top_value, along)), axis=along)
    return (top_value, total_sum)


def shards(images, texts, scale, cotangent):
    row_count = images.shape[0]
    logit_scale = scale[0]
    cot_rows = cotangent[0]
    cot_cols = cotangent[1]
    low_start = jnp.full((row_count,), -1e30, jnp.float32)
    zero_sums = jnp.zeros((row_count,), jnp.float32)
    all_images, all_texts = (
        lax.all_gather(images, "blk", axis=0, tiled=True),
        lax.all_gather(texts, "blk", axis=0, tiled=True),
    )
    batch_total = all_images.shape[0]
    block_width = min(batch_total, 1024)
    block_count = batch_total // block_width

    def first_pass(step, carried):
        row_part, col_part = carried
        text_block = lax.dynamic_slice_in_dim(all_texts, step * block_width, block_width, 0)
        image_block = lax.dynamic_slice_in_dim(all_images, step * block_width, block_width, 0)
        row_scores = logit_scale * dot_rows(text_block, images)
        col_scores = logit_scale * dot_rows(image_block, texts)
        return (
            merge_pair(row_part, block_stats(row_scores, 0)),
            merge_pair(col_part, block_stats(col_scores, 0)),
        )

    row_part, col_part = lax.fori_loop(
        0, block_count, first_pass, ((low_start, zero_sums), (low_start, zero_sums))
    )
    row_lse = row_part[0] + jnp.log(row_part[1])
    col_lse = col_part[0] + jnp.log(col_part[1])
    matched = logit_scale * jnp.sum(images.astype(jnp.float32) * texts.astype(jnp.float32), axis=1)
    row_losses = jnp.stack([row_lse - matched, col_lse - matched])
    all_row_lse, all_col_lse, all_cot_rows, all_cot_cols = (
        lax.all_gather(row_lse, "blk", axis=0, tiled=True),
        lax.all_gather(col_lse, "blk", axis=0, tiled=True),
        lax.all_gather(cot_rows, "blk", axis=0, tiled=True),
        lax.all_gather(cot_cols, "blk", axis=0, tiled=True),
    )

    def second_pass(step, carried):
        acc_images, acc_texts = carried
        start = step * block_width
        text_block = lax.dynamic_slice_in_dim(all_texts, start, block_width, 0)
        image_block = lax.dynamic_slice_in_dim(all_images, start, block_width, 0)
        col_lse_block = lax.dynamic_slice_in_dim(all_col_lse, start, block_width, 0)
        col_cot_block = lax.dynamic_slice_in_dim(all_cot_cols, start, block_width, 0)
        row_lse_block = lax.dynamic_slice_in_dim(all_row_lse, start, block_width, 0)
        row_cot_block = lax.dynamic_slice_in_dim(all_cot_rows, start, block_width, 0)
        row_scores = logit_scale * dot_rows(text_block, images)
        row_weights = cot_rows[None, :] * jnp.exp(row_scores - row_lse[None, :]) + col_cot_block[
            :, None
        ] * jnp.exp(row_scores - col_lse_block[:, None])
        acc_images = acc_images + dot_lead(row_weights.astype(jnp.bfloat16), text_block)
        col_scores = logit_scale * dot_rows(image_block, texts)
        col_weights = row_cot_block[:, None] * jnp.exp(
            col_scores - row_lse_block[:, None]
        ) + cot_cols[None, :] * jnp.exp(col_scores - col_lse[None, :])
        acc_texts = acc_texts + dot_lead(col_weights.astype(jnp.bfloat16), image_block)
        return (acc_images, acc_texts)

    zero_grads = jnp.zeros((row_count, images.shape[1]), jnp.float32)
    image_terms, text_terms = lax.fori_loop(0, block_count, second_pass, (zero_grads, zero_grads))
    both_cot = (cot_rows + cot_cols)[:, None]
    grad_images = logit_scale * (image_terms - both_cot * texts.astype(jnp.float32))
    grad_texts = logit_scale * (text_terms - both_cot * images.astype(jnp.float32))
    return (row_losses, grad_images, grad_texts)


def solution(mesh):
    count = mesh.shape["blk"]

    def step(images, texts, scale, cotangent):
        if count == 2 * LINE and images.shape[0] % LANES == 0:
            return exchange(images, texts, scale, cotangent, count)
        return shards(images, texts, scale, cotangent)

    return jax.shard_map(
        step,
        mesh=mesh,
        in_specs=(P(("dp", "blk"), None), P(("dp", "blk"), None), P(), P(None, ("dp", "blk"))),
        out_specs=(P(None, ("dp", "blk")), P(("dp", "blk"), None), P(("dp", "blk"), None)),
        check_vma=False,
    )
```

```python
import jax
import jax.numpy as jnp
from jax import lax
from jax.experimental import pallas as pl
from jax.experimental.pallas import tpu as pltpu
from jax.sharding import PartitionSpec as P

LANES = 128
VMEM_BYTES = 67043328
MARGIN = 4096
MESH = pl.DeviceIdType.MESH

SLOTS = (
    ((0, 0), (0, 1), (1, 0), (1, 1), (2, 0), (2, 1), (3, 0), (3, 1)),
    ((1, 0), (1, 1), (0, 0), (2, 0), (0, 1), (3, 0), (2, 1), (3, 1)),
)
LINE = len(SLOTS[0]) // 2
PHASES = (
    (
        [
            ("I", (0, 1), "i"), ("I", (1, 0), "x"), ("T", (0, 1), "i"), ("T", (1, 0), "x"),
        ],
        [("I", (1, 1), ""), ("I", (2, 0), "x"), ("T", (1, 1), ""), ("T", (2, 0), "x")],
        [("I", (2, 1), ""), ("I", (3, 0), "x"), ("T", (2, 1), ""), ("T", (3, 0), "")],
        [("I", (3, 1), ""), ("T", (3, 1), "")],
    ),
    (
        [
            ("I", (1, 1), ""), ("I", (0, 0), "i"), ("I", (2, 0), "ox"),
            ("T", (1, 1), ""), ("T", (0, 0), "i"), ("T", (2, 0), "ox"),
        ],
        [
            ("I", (0, 1), ""), ("I", (3, 0), "o"), ("T", (0, 1), ""),
            ("T", (3, 0), "ox"), ("I", (3, 0), "X"),
        ],
        [("I", (2, 1), ""), ("T", (2, 1), "")],
        [("T", (3, 1), "o"), ("I", (3, 1), "")],
    ),
)
GROUPS = ((0, 1), (1, 3), (3, 5), (5, 7), (7, 8))
OWN_WAYS = ("ix", "iox")


def landing(half, block, way):
    place, other = block
    if way == "x":
        return half, (place, 1 - other)
    if way == "o":
        return half - 1, block
    if half == LINE // 2 - 1:
        return half, (LINE - 1 - place, other)
    return half + 1, block


def as_column(row, rows):
    return jnp.transpose(jnp.broadcast_to(row, (LANES, rows)))


def fold(top_ref, sum_ref, tile, low, high, fresh):
    top = jnp.max(tile, axis=0, keepdims=True)
    if fresh:
        sum_ref[:, low:high] = jnp.sum(jnp.exp(tile - top), axis=0, keepdims=True)
    else:
        before = top_ref[:, low:high]
        top = jnp.maximum(before, top)
        sum_ref[:, low:high] = sum_ref[:, low:high] * jnp.exp(before - top) + jnp.sum(
            jnp.exp(tile - top), axis=0, keepdims=True
        )
    top_ref[:, low:high] = top


def kernel(
    scale_ref, images_ref, texts_ref, cot_ref,
    all_images, all_texts, all_cot, weights_i, weights_t, lses_ref,
    strip_i, strip_t, top_r, sum_r, top_c, sum_c, scale_own, send_sem, recv_sem, own_sem,
):
    rows, width = images_ref.shape
    me = lax.axis_index("blk")
    place, column = me // 2, lax.rem(me, 2)
    upper = place // (LINE // 2)
    step = 1 - 2 * upper
    from_end = place + upper * (LINE - 1 - 2 * place)
    peers = {
        "x": place * 2 + 1 - column,
        "i": (place + step) * 2 + column,
        "o": (place - step) * 2 + column,
    }
    kinds = "ITC"

    def part(kind, slot):
        if kind == "C":
            return all_cot.at[slot]
        return (all_images if kind == "I" else all_texts).at[pl.ds(slot * rows, rows)]

    def copy(half, kind, block, way):
        slot = SLOTS[half].index(block)
        there, name = landing(half, block, way)
        own = {"I": images_ref, "T": texts_ref, "C": cot_ref}[kind]
        target = SLOTS[there].index(name)
        at = kinds.index(kind)
        return pltpu.make_async_remote_copy(
            src_ref=own if slot == 0 else part(kind, slot),
            dst_ref=part(kind, target),
            send_sem=send_sem.at[at, slot, "xio".index(way)],
            recv_sem=recv_sem.at[at, target],
            device_id={"blk": peers[way]},
            device_id_type=MESH,
        )

    def arrived(half, kind, block):
        slot = SLOTS[half].index(block)
        at = kinds.index(kind)
        pltpu.make_async_remote_copy(
            src_ref=part(kind, slot),
            dst_ref=part(kind, slot),
            send_sem=send_sem.at[at, slot, 0],
            recv_sem=recv_sem.at[at, slot],
            device_id={"blk": peers["x"]},
            device_id_type=MESH,
        ).wait_recv()

    def both(kind):
        return ("C", "T") if kind == "T" else ("I",)

    sent = ([], [])

    def phase(number):
        for half in range(LINE // 2):

            @pl.when(from_end == half)
            def _():
                for kind, block, ways in PHASES[half][number]:
                    for each in both(kind):
                        if ways != "X":
                            arrived(half, each, block)
                        for way in ways.lower():
                            one = (half, each, block, way)
                            copy(*one).start()
                            sent[half].append(one)

    mine = [
        pltpu.make_async_copy(source, part(kind, 0), own_sem.at[kinds.index(kind)])
        for kind, source in zip(kinds, (images_ref, texts_ref, cot_ref))
    ] + [pltpu.make_async_copy(scale_ref, scale_own, own_sem.at[len(kinds)])]
    barrier = pltpu.get_barrier_semaphore()
    for half in range(LINE // 2):

        @pl.when(from_end == half)
        def _():
            for way in OWN_WAYS[half]:
                pl.semaphore_signal(barrier, inc=1, device_id={"blk": peers[way]}, device_id_type=MESH)
            pl.semaphore_wait(barrier, len(OWN_WAYS[half]))
            for kind in "ICT":
                for way in OWN_WAYS[half]:
                    one = (half, kind, SLOTS[half][0], way)
                    copy(*one).start()
                    sent[half].append(one)

    for each in mine:
        each.start()
    for each in mine:
        each.wait()

    scale = scale_own[...]

    def scores(left, right):
        return scale * dot_rows(left, right)

    def accumulate(left, right, strip, top, total, low, high):
        old, new = low * rows, high * rows
        tile = scores(left[old:new, :], right[0:new, :])
        fold(top, total, tile[:, old:], old, new, True)
        if low == 0:
            strip[:, old:new] = tile
            return
        fold(top, total, tile[:, :old], 0, old, False)
        tile = scores(left[0:old, :], right[old:new, :])
        strip[:, old:new] = tile[0:rows, :]
        fold(top, total, tile, old, new, False)

    for number, (low, high) in enumerate(GROUPS):
        if number:
            phase(number - 1)
        accumulate(all_images, all_texts, strip_i, top_c, sum_c, low, high)
        accumulate(all_texts, all_images, strip_t, top_r, sum_r, low, high)

    row_lse = top_r[...] + jnp.log(sum_r[...])
    col_lse = top_c[...] + jnp.log(sum_c[...])
    own_r, own_c = row_lse[:, 0:rows], col_lse[:, 0:rows]
    lses_ref[0:1, :] = own_r
    lses_ref[1:2, :] = own_c
    lses_ref[2:3, :] = jnp.broadcast_to(scale, (1, rows))
    cot_r, cot_c = all_cot[0, 0:1, :], all_cot[0, 1:2, :]
    own_r_col, own_c_col = as_column(own_r, rows), as_column(own_c, rows)
    cot_r_col, cot_c_col = as_column(cot_r, rows), as_column(cot_c, rows)
    count = all_cot.shape[0]
    for slot in range(count):
        r_row, c_row = all_cot[slot, 0:1, :], all_cot[slot, 1:2, :]
        for at in range(0, rows, LANES):
            span = slice(slot * rows + at, slot * rows + at + LANES)
            part_i, part_t = strip_i[:, span], strip_t[:, span]
            weights_i[:, span] = (
                cot_r_col * jnp.exp(part_i - own_r_col)
                + c_row[:, at : at + LANES] * jnp.exp(part_i - col_lse[:, span])
            ).astype(jnp.bfloat16)
            weights_t[:, span] = (
                r_row[:, at : at + LANES] * jnp.exp(part_t - row_lse[:, span])
                + cot_c_col * jnp.exp(part_t - own_c_col)
            ).astype(jnp.bfloat16)

    for half in range(LINE // 2):

        @pl.when(from_end == half)
        def _():
            for one in sent[half]:
                copy(*one).wait_send()


def finish(
    all_images, all_texts, all_cot, weights_i, weights_t, lses_ref,
    losses_ref, grad_images_ref, grad_texts_ref, losses, grad_images, grad_texts, sem,
):
    rows, width = grad_images.shape
    scale = lses_ref[2:3, 0:LANES]
    both_cot = as_column(all_cot[0, 0:1, :] + all_cot[0, 1:2, :], rows)
    outs = [
        pltpu.make_async_copy(*pair, sem.at[at])
        for at, pair in enumerate(
            ((grad_images, grad_images_ref), (grad_texts, grad_texts_ref), (losses, losses_ref))
        )
    ]
    terms = jnp.dot(weights_i[...], all_texts[...], preferred_element_type=jnp.float32)
    product = jnp.zeros((rows, LANES), jnp.float32)
    for at in range(0, width, LANES):
        span = slice(at, at + LANES)
        text = all_texts[0:rows, span].astype(jnp.float32)
        product = product + all_images[0:rows, span].astype(jnp.float32) * text
        grad_images[:, span] = scale * (terms[:, span] - both_cot * text)
    outs[0].start()
    matched = lses_ref[2:3, :] * jnp.sum(jnp.transpose(product), axis=0, keepdims=True)
    losses[...] = lses_ref[0:2, :] - matched
    outs[2].start()
    terms = jnp.dot(weights_t[...], all_images[...], preferred_element_type=jnp.float32)
    for at in range(0, width, LANES):
        span = slice(at, at + LANES)
        image = all_images[0:rows, span].astype(jnp.float32)
        grad_texts[:, span] = scale * (terms[:, span] - both_cot * image)
    outs[1].start()
    for out in outs:
        out.wait()


def exchange(images, texts, scale, cotangent, count):
    rows, width = images.shape
    total = count * rows
    vmem = pl.BlockSpec(memory_space=pltpu.VMEM)
    hbm = pl.BlockSpec(memory_space=pltpu.HBM)
    f32, bf16 = jnp.float32, jnp.bfloat16
    kept = (
        pltpu.VMEM((total, width), bf16),
        pltpu.VMEM((total, width), bf16),
        pltpu.VMEM((count, 2, rows), f32),
        pltpu.VMEM((rows, total), bf16),
        pltpu.VMEM((rows, total), bf16),
        pltpu.VMEM((3, rows), f32),
    )
    handed_on = 2 * total * (2 * width + 2 * rows) + 4 * 2 * rows * (count + 2)
    grant = VMEM_BYTES - handed_on - MARGIN
    gathered = pl.pallas_call(
        kernel,
        out_shape=kept,
        in_specs=[hbm, hbm, hbm, hbm],
        out_specs=(vmem,) * len(kept),
        scratch_shapes=[
            pltpu.VMEM((rows, total), f32),
            pltpu.VMEM((rows, total), f32),
            pltpu.VMEM((1, total), f32),
            pltpu.VMEM((1, total), f32),
            pltpu.VMEM((1, total), f32),
            pltpu.VMEM((1, total), f32),
            pltpu.VMEM((1, 1), f32),
            pltpu.SemaphoreType.DMA((3, count, 3)),
            pltpu.SemaphoreType.DMA((3, count)),
            pltpu.SemaphoreType.DMA((4,)),
        ],
        compiler_params=pltpu.CompilerParams(
            collective_id=0, has_side_effects=True, vmem_limit_bytes=grant
        ),
    )(scale.reshape(1, 1), images, texts, cotangent)
    outs = (
        jax.ShapeDtypeStruct((2, rows), f32),
        jax.ShapeDtypeStruct((rows, width), f32),
        jax.ShapeDtypeStruct((rows, width), f32),
    )
    return pl.pallas_call(
        finish,
        out_shape=outs,
        in_specs=[vmem] * len(kept),
        out_specs=(hbm,) * len(outs),
        scratch_shapes=[pltpu.VMEM(out.shape, f32) for out in outs] + [pltpu.SemaphoreType.DMA((3,))],
        compiler_params=pltpu.CompilerParams(vmem_limit_bytes=grant // 2),
    )(*gathered)


def dot_rows(left, right):
    return lax.dot_general(
        left, right, (((1,), (1,)), ((), ())), preferred_element_type=jnp.float32
    )


def dot_lead(left, right):
    return lax.dot_general(
        left, right, (((0,), (0,)), ((), ())), preferred_element_type=jnp.float32
    )


def merge_pair(first, second):
    max_new = jnp.maximum(first[0], second[0])
    return (
        max_new,
        first[1] * jnp.exp(first[0] - max_new) + second[1] * jnp.exp(second[0] - max_new),
    )


def block_stats(scores, along):
    top_value = jnp.max(scores, axis=along)
    total_sum = jnp.sum(jnp.exp(scores - jnp.expand_dims(top_value, along)), axis=along)
    return (top_value, total_sum)


def shards(images, texts, scale, cotangent):
    row_count = images.shape[0]
    logit_scale = scale[0]
    cot_rows = cotangent[0]
    cot_cols = cotangent[1]
    low_start = jnp.full((row_count,), -1e30, jnp.float32)
    zero_sums = jnp.zeros((row_count,), jnp.float32)
    all_images, all_texts = (
        lax.all_gather(images, "blk", axis=0, tiled=True),
        lax.all_gather(texts, "blk", axis=0, tiled=True),
    )
    batch_total = all_images.shape[0]
    block_width = min(batch_total, 1024)
    block_count = batch_total // block_width

    def first_pass(step, carried):
        row_part, col_part = carried
        text_block = lax.dynamic_slice_in_dim(all_texts, step * block_width, block_width, 0)
        image_block = lax.dynamic_slice_in_dim(all_images, step * block_width, block_width, 0)
        row_scores = logit_scale * dot_rows(text_block, images)
        col_scores = logit_scale * dot_rows(image_block, texts)
        return (
            merge_pair(row_part, block_stats(row_scores, 0)),
            merge_pair(col_part, block_stats(col_scores, 0)),
        )

    row_part, col_part = lax.fori_loop(
        0, block_count, first_pass, ((low_start, zero_sums), (low_start, zero_sums))
    )
    row_lse = row_part[0] + jnp.log(row_part[1])
    col_lse = col_part[0] + jnp.log(col_part[1])
    matched = logit_scale * jnp.sum(images.astype(jnp.float32) * texts.astype(jnp.float32), axis=1)
    row_losses = jnp.stack([row_lse - matched, col_lse - matched])
    all_row_lse, all_col_lse, all_cot_rows, all_cot_cols = (
        lax.all_gather(row_lse, "blk", axis=0, tiled=True),
        lax.all_gather(col_lse, "blk", axis=0, tiled=True),
        lax.all_gather(cot_rows, "blk", axis=0, tiled=True),
        lax.all_gather(cot_cols, "blk", axis=0, tiled=True),
    )

    def second_pass(step, carried):
        acc_images, acc_texts = carried
        start = step * block_width
        text_block = lax.dynamic_slice_in_dim(all_texts, start, block_width, 0)
        image_block = lax.dynamic_slice_in_dim(all_images, start, block_width, 0)
        col_lse_block = lax.dynamic_slice_in_dim(all_col_lse, start, block_width, 0)
        col_cot_block = lax.dynamic_slice_in_dim(all_cot_cols, start, block_width, 0)
        row_lse_block = lax.dynamic_slice_in_dim(all_row_lse, start, block_width, 0)
        row_cot_block = lax.dynamic_slice_in_dim(all_cot_rows, start, block_width, 0)
        row_scores = logit_scale * dot_rows(text_block, images)
        row_weights = cot_rows[None, :] * jnp.exp(row_scores - row_lse[None, :]) + col_cot_block[
            :, None
        ] * jnp.exp(row_scores - col_lse_block[:, None])
        acc_images = acc_images + dot_lead(row_weights.astype(jnp.bfloat16), text_block)
        col_scores = logit_scale * dot_rows(image_block, texts)
        col_weights = row_cot_block[:, None] * jnp.exp(
            col_scores - row_lse_block[:, None]
        ) + cot_cols[None, :] * jnp.exp(col_scores - col_lse[None, :])
        acc_texts = acc_texts + dot_lead(col_weights.astype(jnp.bfloat16), image_block)
        return (acc_images, acc_texts)

    zero_grads = jnp.zeros((row_count, images.shape[1]), jnp.float32)
    image_terms, text_terms = lax.fori_loop(0, block_count, second_pass, (zero_grads, zero_grads))
    both_cot = (cot_rows + cot_cols)[:, None]
    grad_images = logit_scale * (image_terms - both_cot * texts.astype(jnp.float32))
    grad_texts = logit_scale * (text_terms - both_cot * images.astype(jnp.float32))
    return (row_losses, grad_images, grad_texts)


def solution(mesh):
    count = mesh.shape["blk"]

    def step(images, texts, scale, cotangent):
        if count == 2 * LINE and images.shape[0] % LANES == 0:
            return exchange(images, texts, scale, cotangent, count)
        return shards(images, texts, scale, cotangent)

    return jax.shard_map(
        step,
        mesh=mesh,
        in_specs=(P(("dp", "blk"), None), P(("dp", "blk"), None), P(), P(None, ("dp", "blk"))),
        out_specs=(P(None, ("dp", "blk")), P(("dp", "blk"), None), P(("dp", "blk"), None)),
        check_vma=False,
    )
```
